512 devices in a mesh: cfg: 2 (over y), expert: 64 (over z, core), ffn: 4 (over x).
Axes of the slice: x: 4, y: 2, z: 32, core: 2. Of those that a mesh axis runs over, the one named last changes fastest.
The devices are a block of a 4x8x32 slice.
Arguments:
- tokens: bfloat16 [32768, 2048], P(('cfg', 'expert'), 'ffn'), parts along dimension 0, may hold values from -6 to 6
- chosen: int32 [128, 512], P(('cfg', 'expert')), parts along dimension 0, may hold values from 0 to 16383, as said below
- gates: float32 [128, 512], P(('cfg', 'expert')), parts along dimension 0, may hold values from 0.1 to 1
- capacity: int32 [2], P('cfg'), parts along dimension 0, may hold values from 256 to 512
- w_gate: bfloat16 [64, 2048, 1024], P('expert', None, 'ffn'), may hold values from -0.125 to 0.125
- w_up: bfloat16 [64, 2048, 1024], P('expert', None, 'ffn'), may hold values from -0.125 to 0.125
- w_down: bfloat16 [64, 1024, 2048], P('expert', 'ffn'), may hold values from -0.1875 to 0.1875
Outputs:
- mixed: bfloat16 [32768, 2048], P(('cfg', 'expert'), 'ffn'), parts along dimension 0
The draws below stay inside these ranges and needn't reach their ends.
There are 2 independent parts, one for each index of `cfg`. The reference program is written for one: setup_inputs(seed, part) draws one part's arguments, and reference() takes and returns one part's arrays. A program takes and returns all parts, laid end to end along the dimension named above; an argument that names none is the same for every part. Nothing has to cross between parts.
Inputs may be any that keep to these rules, and one draw needn't show every extreme that they name: `chosen`: each row lists 512 different tokens; at most 16 of one row's tokens lie in one aligned block of 256 tokens, and every row has exactly 16 in some block.
All inputs are finite; a program needn't handle non-finite values.
Results may differ from the reference program's by a relative error of at most 0.013.
Values may be sent and summed in bfloat16 or wider, within the bound.
No kernel may reach another device: no remote copies, remote signals or barrier semaphores. Data moves between devices by JAX's collectives and lax.ppermute only.
A program may use at most 64 MiB of HBM per device.

```python
import math
import jax
import jax.numpy as jnp
from jax import lax

D = 2048
FF = 1024
TOK_DEV = 256
FF_DEV = 256
EXPERTS = 64
TOKENS = 16384
CAP = 512
N_FFN = 4


def draw_chosen(key, part):
    half_most = CAP // EXPERTS

    def one_expert(expert_key):
        key_counts, key_sources, key_tokens, key_order = jax.random.split(expert_key, 4)
        shifts = jax.random.randint(key_counts, (EXPERTS // 2,), 0, half_most + 1)
        shifts = shifts.at[0].set(half_most)
        paired = jnp.stack([shifts, -shifts], axis=1).reshape(-1)
        source_order = jax.random.permutation(key_sources, EXPERTS)
        counts = jnp.zeros((EXPERTS,), jnp.int32).at[source_order].set((half_most + paired).astype(jnp.int32))
        token_orders = jax.vmap(lambda inner: jax.random.permutation(inner, TOK_DEV))(jax.random.split(key_tokens, EXPERTS))
        ends = jnp.cumsum(counts)
        starts = ends - counts
        positions = jnp.arange(CAP, dtype=jnp.int32)
        source = jnp.sum((positions[:, None] >= ends[None, :]).astype(jnp.int32), axis=1)
        within = positions - starts[source]
        token_ids = source * TOK_DEV + token_orders[source, within]
        shuffle = jax.random.permutation(key_order, CAP)
        return token_ids[shuffle].astype(jnp.int32)
    expert_keys = jax.random.split(jax.random.fold_in(key, 11), EXPERTS)
    return jax.vmap(one_expert)(expert_keys)


def block_scale(rng, shape, pieces, least, largest):
    gain = 1.0
    for axis_at, shards_of in pieces:
        heights = jax.random.uniform(jax.random.fold_in(jax.random.fold_in(rng, 6), axis_at), (shards_of,), jnp.float32, least / len(pieces), largest / len(pieces))
        gain = gain * jnp.repeat(jnp.exp(heights), shape[axis_at] // shards_of).reshape((-1,) + (1,) * (len(shape) - 1 - axis_at))
    return gain


def centred(key, extent, deviation, reach, cuts=(), held_as=jnp.bfloat16):
    drawn = deviation * jax.random.normal(key, extent, jnp.float32)
    if cuts:
        drawn = drawn * block_scale(key, extent, cuts, -0.22, 0.18)
    return jnp.clip(drawn, -reach, reach).astype(held_as)


def setup_inputs(seed: int = 0, part: int = 0) -> dict:
    key_list = jax.random.split(jax.random.key(seed), 8)
    part_keys = jax.random.split(jax.random.fold_in(key_list[7], part), 8)
    tokens = centred(part_keys[0], (TOKENS, D), 1.0, 6.0, ((0, 64), (1, 4)))
    chosen = draw_chosen(jax.random.fold_in(jax.random.fold_in(key_list[7], part), 71), part)
    gates = jnp.clip(jnp.exp(math.log(1.0) - 2.3025851 * jax.random.uniform(part_keys[2], (EXPERTS, CAP), jnp.float32) ** block_scale(part_keys[2], (EXPERTS, CAP), ((0, 64),), -0.2, 0.2)), 0.1, 1.0)
    capacity = jax.random.randint(part_keys[3], (1,), CAP // 2, CAP + 1).astype(jnp.int32)
    w_gate = centred(key_list[4], (EXPERTS, D, FF), D ** -0.5, 0.125, ((0, 64), (2, 4)))
    w_up = centred(key_list[5], (EXPERTS, D, FF), D ** -0.5, 0.125, ((0, 64), (2, 4)))
    w_down = centred(key_list[6], (EXPERTS, FF, D), FF ** -0.5, 0.1875, ((0, 64), (1, 4)))
    return {"tokens": tokens, "chosen": chosen, "gates": gates, "capacity": capacity, "w_gate": w_gate, "w_up": w_up, "w_down": w_down}


def reference(tokens, chosen, gates, capacity, w_gate, w_up, w_down):
    positions = jnp.arange(CAP, dtype=jnp.int32)
    live = jnp.where(positions[None, :] < capacity[0], gates, jnp.zeros_like(gates)).astype(jnp.float32)

    def expert_step(total, item):
        picked_ids, weights, gate_cols, up_cols, down_rows = item
        gathered = jnp.take(tokens, picked_ids, axis=0)
        summed = jnp.zeros((CAP, D), jnp.float32)
        for block in range(N_FFN):
            low_col = block * FF_DEV
            gate_part = jnp.dot(gathered, gate_cols[:, low_col:low_col + FF_DEV], preferred_element_type=jnp.float32)
            up_part = jnp.dot(gathered, up_cols[:, low_col:low_col + FF_DEV], preferred_element_type=jnp.float32)
            hidden = (jax.nn.silu(gate_part) * up_part).astype(jnp.bfloat16)
            partial_value = jnp.dot(hidden, down_rows[low_col:low_col + FF_DEV, :], preferred_element_type=jnp.float32).astype(jnp.bfloat16)
            summed = summed + lax.optimization_barrier(partial_value).astype(jnp.float32)
        contribution = (weights[:, None] * summed).astype(jnp.bfloat16)
        total = total.at[picked_ids].add(lax.optimization_barrier(contribution).astype(jnp.float32))
        return total, None

    start_total = jnp.zeros((TOKENS, D), jnp.float32)
    total, unused = lax.scan(expert_step, start_total, (chosen, live, w_gate, w_up, w_down))
    return total.astype(jnp.bfloat16)
```

```python
import jax
import jax.numpy as jnp
from jax import lax
from jax.sharding import Mesh
from jax.sharding import PartitionSpec as P

EXPERT = ("expert_0", "expert_1")
CFG_EXPERT = ("cfg", "expert_0", "expert_1")
CHUNKS = 2


def hop(array, axis, step):
    peers = lax.axis_size(axis)
    return lax.ppermute(array, axis, [(k, (k + step) % peers) for k in range(peers)])


def one_hot(rows, columns):
    return (rows[:, None] == columns[None, :]).astype(jnp.bfloat16)


def mm(a, b):
    return jnp.dot(a, b, preferred_element_type=jnp.float32)


def swap(tiles):
    return lax.all_to_all(tiles, EXPERT, split_axis=0, concat_axis=0, tiled=True)


def shards(tokens, chosen, gates, capacity, w_gate, w_up, w_down):
    experts_n = lax.axis_size(EXPERT)
    ffn_n = lax.axis_size("ffn")
    tok_dev, width = tokens.shape
    picked_ids = chosen[0]
    listed = picked_ids.shape[0]
    slot_depth = 2 * listed // experts_n
    slots_n = experts_n * slot_depth
    part = width // CHUNKS

    positions = jnp.arange(listed, dtype=jnp.int32)
    alive = positions < capacity[0]
    weights = jnp.where(alive, gates[0], jnp.zeros_like(gates[0]))
    source = picked_ids // tok_dev
    offset = picked_ids - source * tok_dev
    member = (source[:, None] == jnp.arange(experts_n, dtype=jnp.int32)[None, :]).astype(jnp.int32)
    before = jnp.cumsum(member, axis=0) - member
    rank_in = jnp.sum(before * member, axis=1)
    slot_of = source * slot_depth + rank_in
    wanted = jnp.where(alive, offset, -1)
    request = jnp.full((slots_n,), -1, jnp.int32).at[slot_of].set(wanted)
    requested = swap(request.reshape(experts_n, slot_depth)).reshape(-1)

    selects = one_hot(requested, jnp.arange(tok_dev, dtype=jnp.int32))
    slots_at = one_hot(jnp.arange(slots_n, dtype=jnp.int32), slot_of)
    take_at = one_hot(slot_of, jnp.arange(slots_n, dtype=jnp.int32))

    me = lax.axis_index("ffn")

    def turned(blocks):
        return [
            lax.dynamic_index_in_dim(blocks, lax.rem(me + j, ffn_n), 0, keepdims=False)
            for j in range(ffn_n)
        ]

    gate_rows = turned(w_gate[0].reshape(ffn_n, width, -1))
    up_rows = turned(w_up[0].reshape(ffn_n, width, -1))
    down_cols = turned(jnp.moveaxis(w_down[0].reshape(-1, ffn_n, width), 1, 0))

    gate_sum = 0.0
    up_sum = 0.0
    for c in range(CHUNKS):
        cols = slice(c * part, (c + 1) * part)
        rows = mm(selects, tokens[:, cols]).astype(jnp.bfloat16)
        slots = swap(rows.reshape(experts_n, slot_depth, part)).reshape(slots_n, part)
        picked = mm(take_at, slots).astype(jnp.bfloat16)
        for j in range(ffn_n):
            held = hop(picked, "ffn", -j) if j else picked
            gate_sum = gate_sum + mm(held, gate_rows[j][cols])
            up_sum = up_sum + mm(held, up_rows[j][cols])
    hidden = (jax.nn.silu(gate_sum) * up_sum).astype(jnp.bfloat16)

    outs = []
    for c in range(CHUNKS):
        cols = slice(c * part, (c + 1) * part)
        summed = 0.0
        for j in range(ffn_n):
            piece = mm(hidden, down_cols[j][:, cols]).astype(jnp.bfloat16)
            piece = hop(piece, "ffn", j) if j else piece
            summed = summed + piece.astype(jnp.float32)
        contribution = (weights[:, None] * summed).astype(jnp.bfloat16)
        back = mm(slots_at, contribution).astype(jnp.bfloat16)
        back = swap(back.reshape(experts_n, slot_depth, part)).reshape(slots_n, part)
        outs.append(
            lax.dot_general(
                selects, back, (((0,), (0,)), ((), ())), preferred_element_type=jnp.float32
            ).astype(jnp.bfloat16)
        )
    return jnp.concatenate(outs, axis=1)


def solution(mesh):
    split = Mesh(
        mesh.devices.reshape(
            mesh.shape["cfg"], mesh.shape["expert"] // 2, 2, mesh.shape["ffn"]
        ),
        ("cfg", "expert_0", "expert_1", "ffn"),
    )
    return jax.shard_map(
        shards,
        mesh=split,
        in_specs=(
            P(CFG_EXPERT, "ffn"),
            P(CFG_EXPERT, None),
            P(CFG_EXPERT, None),
            P("cfg"),
            P(EXPERT, None, "ffn"),
            P(EXPERT, None, "ffn"),
            P(EXPERT, "ffn", None),
        ),
        out_specs=P(CFG_EXPERT, "ffn"),
        check_vma=False,
    )
```

```python
import jax
import jax.numpy as jnp
from jax import lax
from jax.sharding import Mesh
from jax.sharding import PartitionSpec as P


EXPERT = ("expert_0", "expert_1")
CFG_EXPERT = ("cfg", "expert_0", "expert_1")


def hop(array, step):
    peers = lax.axis_size("ffn")
    return lax.ppermute(array, "ffn", [(k, (k + step) % peers) for k in range(peers)])


def one_hot(rows, columns):
    return (rows[:, None] == columns[None, :]).astype(jnp.bfloat16)


def mm(a, b):
    return jnp.dot(a, b, preferred_element_type=jnp.float32)


def swap(tiles):
    return lax.all_to_all(tiles, EXPERT, split_axis=0, concat_axis=0, tiled=True)


def shards(tokens, chosen, gates, capacity, w_gate, w_up, w_down):
    experts_n = lax.axis_size(EXPERT)
    ffn_n = lax.axis_size("ffn")
    me = lax.axis_index("ffn")
    tok_dev, width = tokens.shape
    picked_ids = chosen[0]
    listed = picked_ids.shape[0]
    slot_depth = 2 * listed // experts_n
    depth = slot_depth // ffn_n
    held = experts_n * depth

    positions = jnp.arange(listed, dtype=jnp.int32)
    alive = positions < capacity[0]
    weights = jnp.where(alive, gates[0], jnp.zeros_like(gates[0]))
    source = picked_ids // tok_dev
    offset = picked_ids - source * tok_dev
    member = one_hot(source, jnp.arange(experts_n, dtype=jnp.int32))
    earlier = (positions[:, None] > positions[None, :]).astype(jnp.bfloat16)
    before = mm(earlier, member)
    rank_in = jnp.sum(before * member.astype(jnp.float32), axis=1).astype(jnp.int32)
    place_in = (rank_in % ffn_n) * depth + rank_in // ffn_n
    asked = jnp.where(alive, offset + 1, 0).astype(jnp.bfloat16)
    spread = one_hot(place_in, jnp.arange(slot_depth, dtype=jnp.int32)) * asked[:, None]
    request = lax.dot_general(
        member, spread, (((0,), (0,)), ((), ())), preferred_element_type=jnp.float32
    )
    request = request.astype(jnp.int32) - 1
    requested = swap(request.reshape(experts_n, 1, slot_depth))
    requested = requested.reshape(experts_n, ffn_n, depth)

    pieces = jnp.stack([tokens, hop(tokens, 1), hop(tokens, 2), hop(tokens, -1)])

    mine = lax.dynamic_index_in_dim(requested, me, 1, keepdims=False).reshape(-1)
    selects = one_hot(mine, jnp.arange(tok_dev, dtype=jnp.int32))
    rows = jnp.concatenate(
        [
            mm(
                selects,
                lax.dynamic_index_in_dim(pieces, lax.rem(me + ffn_n - b, ffn_n), 0, keepdims=False),
            ).astype(jnp.bfloat16)
            for b in range(ffn_n)
        ],
        axis=1,
    )
    rows, shared = lax.optimization_barrier((rows, (w_gate[0], w_up[0], w_down[0])))
    arrived = swap(rows.reshape(experts_n, depth, -1)).reshape(held, -1)

    own_gate, _, _ = shared
    half = own_gate.shape[1] // 2
    left = [hop(w, 1) for w in shared]
    right = [hop(w, -1) for w in shared]
    far_left = [hop(left[0][:, :half], 1), hop(left[1][:, :half], 1), hop(left[2][:half], 1)]
    far_right = [hop(right[0][:, half:], -1), hop(right[1][:, half:], -1), hop(right[2][half:], -1)]

    slot_of = source * depth + rank_in // ffn_n
    at_mine = (rank_in % ffn_n) == me
    gate_of = jnp.sum(
        jnp.where(
            (jnp.arange(held, dtype=jnp.int32)[:, None] == slot_of[None, :])
            & at_mine[None, :],
            weights[None, :],
            0.0,
        ),
        axis=1,
    )

    summed = 0.0
    for gate_cols, up_cols, down_rows in (shared, left, right, far_left, far_right):
        gate_part = mm(arrived, gate_cols)
        up_part = mm(arrived, up_cols)
        hidden = (jax.nn.silu(gate_part) * up_part).astype(jnp.bfloat16)
        summed = summed + mm(hidden, down_rows)
    contribution = (gate_of[:, None] * summed).astype(jnp.bfloat16)
    returned = swap(contribution.reshape(experts_n, depth, -1))

    tiles = jnp.moveaxis(returned.reshape(held, ffn_n, width), 1, 0)
    tiles = lax.all_to_all(tiles, "ffn", split_axis=0, concat_axis=0, tiled=True)
    slot_token = jnp.moveaxis(requested, 1, 0).reshape(-1)
    placement = one_hot(jnp.arange(tok_dev, dtype=jnp.int32), slot_token)
    return mm(placement, tiles.reshape(ffn_n * held, width)).astype(jnp.bfloat16)


def solution(mesh):
    split = Mesh(
        mesh.devices.reshape(
            mesh.shape["cfg"], mesh.shape["expert"] // 2, 2, mesh.shape["ffn"]
        ),
        ("cfg", "expert_0", "expert_1", "ffn"),
    )
    return jax.shard_map(
        shards,
        mesh=split,
        in_specs=(
            P(CFG_EXPERT, "ffn"),
            P(CFG_EXPERT, None),
            P(CFG_EXPERT, None),
            P("cfg"),
            P(EXPERT, None, "ffn"),
            P(EXPERT, None, "ffn"),
            P(EXPERT, "ffn", None),
        ),
        out_specs=P(CFG_EXPERT, "ffn"),
        check_vma=False,
    )
```

```python
import jax
import jax.numpy as jnp
from jax import lax
from jax.sharding import Mesh
from jax.sharding import PartitionSpec as P


EXPERT = ("expert_0", "expert_1")
CFG_EXPERT = ("cfg", "expert_0", "expert_1")


def hop(array, step):
    peers = lax.axis_size("ffn")
    return lax.ppermute(array, "ffn", [(k, (k + step) % peers) for k in range(peers)])


def one_hot(rows, columns):
    return (rows[:, None] == columns[None, :]).astype(jnp.bfloat16)


def mm(a, b):
    return jnp.dot(a, b, preferred_element_type=jnp.float32)


def swap(tiles):
    return lax.all_to_all(tiles, EXPERT, split_axis=0, concat_axis=0, tiled=True)


def shards(tokens, chosen, gates, capacity, w_gate, w_up, w_down):
    experts_n = lax.axis_size(EXPERT)
    ffn_n = lax.axis_size("ffn")
    me = lax.axis_index("ffn")
    tok_dev, width = tokens.shape
    picked_ids = chosen[0]
    listed = picked_ids.shape[0]
    slot_depth = 2 * listed // experts_n
    depth = slot_depth // ffn_n
    held = experts_n * depth

    positions = jnp.arange(listed, dtype=jnp.int32)
    alive = positions < capacity[0]
    weights = jnp.where(alive, gates[0], jnp.zeros_like(gates[0]))
    source = picked_ids // tok_dev
    offset = picked_ids - source * tok_dev
    member = one_hot(source, jnp.arange(experts_n, dtype=jnp.int32))
    earlier = (positions[:, None] > positions[None, :]).astype(jnp.bfloat16)
    before = mm(earlier, member)
    rank_in = jnp.sum(before * member.astype(jnp.float32), axis=1).astype(jnp.int32)
    place_in = (rank_in % ffn_n) * depth + rank_in // ffn_n
    asked = jnp.where(alive, offset + 1, 0).astype(jnp.bfloat16)
    spread = one_hot(place_in, jnp.arange(slot_depth, dtype=jnp.int32)) * asked[:, None]
    request = lax.dot_general(
        member, spread, (((0,), (0,)), ((), ())), preferred_element_type=jnp.float32
    )
    request = request.astype(jnp.int32) - 1
    requested = swap(request.reshape(experts_n, 1, slot_depth))
    requested = requested.reshape(experts_n, ffn_n, depth)

    pieces = jnp.stack([tokens, hop(tokens, 1), hop(tokens, 2), hop(tokens, -1)])

    mine = lax.dynamic_index_in_dim(requested, me, 1, keepdims=False).reshape(-1)
    selects = one_hot(mine, jnp.arange(tok_dev, dtype=jnp.int32))
    rows = jnp.concatenate(
        [
            mm(
                selects,
                lax.dynamic_index_in_dim(pieces, lax.rem(me + ffn_n - b, ffn_n), 0, keepdims=False),
            ).astype(jnp.bfloat16)
            for b in range(ffn_n)
        ],
        axis=1,
    )
    rows, shared = lax.optimization_barrier((rows, (w_gate[0], w_up[0], w_down[0])))
    arrived = swap(rows.reshape(experts_n, depth, -1)).reshape(held, -1)

    own_gate, _, _ = shared
    half = own_gate.shape[1] // 2
    left = [hop(w, 1) for w in shared]
    right = [hop(w, -1) for w in shared]
    far_left = [hop(left[0][:, :half], 1), hop(left[1][:, :half], 1), hop(left[2][:half], 1)]
    far_right = [hop(right[0][:, half:], -1), hop(right[1][:, half:], -1), hop(right[2][half:], -1)]

    slot_of = source * depth + rank_in // ffn_n
    at_mine = (rank_in % ffn_n) == me
    gate_of = jnp.sum(
        jnp.where(
            (jnp.arange(held, dtype=jnp.int32)[:, None] == slot_of[None, :])
            & at_mine[None, :],
            weights[None, :],
            0.0,
        ),
        axis=1,
    )

    joined = []
    for k, dim in ((0, 1), (1, 1), (2, 0)):
        parts = [g[k] for g in (shared, left, right, far_left, far_right)]
        joined.append(jnp.concatenate(parts, axis=dim))
    gate_cols, up_cols, down_rows = lax.optimization_barrier(tuple(joined))
    hidden = (jax.nn.silu(mm(arrived, gate_cols)) * mm(arrived, up_cols)).astype(jnp.bfloat16)
    summed = mm(hidden, down_rows)
    contribution = (gate_of[:, None] * summed).astype(jnp.bfloat16)
    returned = swap(contribution.reshape(experts_n, depth, -1))

    tiles = jnp.moveaxis(returned.reshape(held, ffn_n, width), 1, 0)
    tiles = lax.all_to_all(tiles, "ffn", split_axis=0, concat_axis=0, tiled=True)
    slot_token = jnp.moveaxis(requested, 1, 0).reshape(-1)
    placement = one_hot(jnp.arange(tok_dev, dtype=jnp.int32), slot_token)
    return mm(placement, tiles.reshape(ffn_n * held, width)).astype(jnp.bfloat16)


def solution(mesh):
    split = Mesh(
        mesh.devices.reshape(
            mesh.shape["cfg"], mesh.shape["expert"] // 2, 2, mesh.shape["ffn"]
        ),
        ("cfg", "expert_0", "expert_1", "ffn"),
    )
    return jax.shard_map(
        shards,
        mesh=split,
        in_specs=(
            P(CFG_EXPERT, "ffn"),
            P(CFG_EXPERT, None),
            P(CFG_EXPERT, None),
            P("cfg"),
            P(EXPERT, None, "ffn"),
            P(EXPERT, None, "ffn"),
            P(EXPERT, "ffn", None),
        ),
        out_specs=P(CFG_EXPERT, "ffn"),
        check_vma=False,
    )
```

```python
import jax
import jax.numpy as jnp
from jax import lax
from jax.sharding import Mesh
from jax.sharding import PartitionSpec as P


EXPERT = ("expert_0", "expert_1")
CFG_EXPERT = ("cfg", "expert_0", "expert_1")


def hop(array, step):
    peers = lax.axis_size("ffn")
    return lax.ppermute(array, "ffn", [(k, (k + step) % peers) for k in range(peers)])


def one_hot(rows, columns):
    return (rows[:, None] == columns[None, :]).astype(jnp.bfloat16)


def mm(a, b):
    return jnp.dot(a, b, preferred_element_type=jnp.float32)


def swap(tiles):
    return lax.all_to_all(tiles, EXPERT, split_axis=0, concat_axis=0, tiled=True)


def shards(tokens, chosen, gates, capacity, w_gate, w_up, w_down):
    experts_n = lax.axis_size(EXPERT)
    ffn_n = lax.axis_size("ffn")
    me = lax.axis_index("ffn")
    tok_dev, width = tokens.shape
    picked_ids = chosen[0]
    listed = picked_ids.shape[0]
    slot_depth = 2 * listed // experts_n
    depth = slot_depth // ffn_n
    held = experts_n * depth

    positions = jnp.arange(listed, dtype=jnp.int32)
    alive = positions < capacity[0]
    weights = jnp.where(alive, gates[0], jnp.zeros_like(gates[0]))
    source = picked_ids // tok_dev
    offset = picked_ids - source * tok_dev
    member = one_hot(source, jnp.arange(experts_n, dtype=jnp.int32))
    earlier = (positions[:, None] > positions[None, :]).astype(jnp.bfloat16)
    before = mm(earlier, member)
    rank_in = jnp.sum(before * member.astype(jnp.float32), axis=1).astype(jnp.int32)
    place_in = (rank_in % ffn_n) * depth + rank_in // ffn_n
    asked = jnp.where(alive, offset + 1, 0).astype(jnp.bfloat16)
    spread = one_hot(place_in, jnp.arange(slot_depth, dtype=jnp.int32)) * asked[:, None]
    request = lax.dot_general(
        member, spread, (((0,), (0,)), ((), ())), preferred_element_type=jnp.float32
    )
    request = request.astype(jnp.int32) - 1
    requested = swap(request.reshape(experts_n, 1, slot_depth))
    requested = requested.reshape(experts_n, ffn_n, depth)

    pieces = jnp.stack([tokens, hop(tokens, 1), hop(tokens, 2), hop(tokens, -1)])

    mine = lax.dynamic_index_in_dim(requested, me, 1, keepdims=False).reshape(-1)
    selects = one_hot(mine, jnp.arange(tok_dev, dtype=jnp.int32))
    rows = jnp.concatenate(
        [
            mm(
                selects,
                lax.dynamic_index_in_dim(pieces, lax.rem(me + ffn_n - b, ffn_n), 0, keepdims=False),
            ).astype(jnp.bfloat16)
            for b in range(ffn_n)
        ],
        axis=1,
    )
    rows, own_down = lax.optimization_barrier((rows, w_down[0]))
    arrived = swap(rows.reshape(experts_n, depth, -1)).reshape(held, -1)

    own_gate, own_up = w_gate[0], w_up[0]
    shared = [own_gate, own_up, own_down]
    half = own_gate.shape[1] // 2
    left = [hop(own_gate, 1), hop(own_up, 1)]
    right = [hop(own_gate, -1), hop(own_up, -1)]
    left.append(hop(own_down, 1))
    right.append(hop(own_down, -1))
    far_left = [hop(left[0][:, :half], 1), hop(left[1][:, :half], 1), hop(left[2][:half], 1)]
    far_right = [hop(right[0][:, half:], -1), hop(right[1][:, half:], -1), hop(right[2][half:], -1)]

    slot_of = source * depth + rank_in // ffn_n
    at_mine = (rank_in % ffn_n) == me
    gate_of = jnp.sum(
        jnp.where(
            (jnp.arange(held, dtype=jnp.int32)[:, None] == slot_of[None, :])
            & at_mine[None, :],
            weights[None, :],
            0.0,
        ),
        axis=1,
    )

    joined = []
    for k, dim in ((0, 1), (1, 1), (2, 0)):
        parts = [g[k] for g in (shared, left, right, far_left, far_right)]
        joined.append(jnp.concatenate(parts, axis=dim))
    gate_cols, up_cols, down_rows = lax.optimization_barrier(tuple(joined))
    hidden = (jax.nn.silu(mm(arrived, gate_cols)) * mm(arrived, up_cols)).astype(jnp.bfloat16)
    summed = mm(hidden, down_rows)
    contribution = (gate_of[:, None] * summed).astype(jnp.bfloat16)
    returned = swap(contribution.reshape(experts_n, depth, -1))

    tiles = jnp.moveaxis(returned.reshape(held, ffn_n, width), 1, 0)
    tiles = lax.all_to_all(tiles, "ffn", split_axis=0, concat_axis=0, tiled=True)
    slot_token = jnp.moveaxis(requested, 1, 0).reshape(-1)
    placement = one_hot(jnp.arange(tok_dev, dtype=jnp.int32), slot_token)
    return mm(placement, tiles.reshape(ffn_n * held, width)).astype(jnp.bfloat16)


def solution(mesh):
    split = Mesh(
        mesh.devices.reshape(
            mesh.shape["cfg"], mesh.shape["expert"] // 2, 2, mesh.shape["ffn"]
        ),
        ("cfg", "expert_0", "expert_1", "ffn"),
    )
    return jax.shard_map(
        shards,
        mesh=split,
        in_specs=(
            P(CFG_EXPERT, "ffn"),
            P(CFG_EXPERT, None),
            P(CFG_EXPERT, None),
            P("cfg"),
            P(EXPERT, None, "ffn"),
            P(EXPERT, None, "ffn"),
            P(EXPERT, "ffn", None),
        ),
        out_specs=P(CFG_EXPERT, "ffn"),
        check_vma=False,
    )
```

```python
import jax
import jax.numpy as jnp
from jax import lax
from jax.sharding import Mesh
from jax.sharding import PartitionSpec as P


EXPERT = ("expert_0", "expert_1")
CFG_EXPERT = ("cfg", "expert_0", "expert_1")


def hop(array, step):
    peers = lax.axis_size("ffn")
    return lax.ppermute(array, "ffn", [(k, (k + step) % peers) for k in range(peers)])


def one_hot(rows, columns):
    return (rows[:, None] == columns[None, :]).astype(jnp.bfloat16)


def mm(a, b):
    return jnp.dot(a, b, preferred_element_type=jnp.float32)


def swap(tiles):
    return lax.all_to_all(tiles, EXPERT, split_axis=0, concat_axis=0, tiled=True)


def shards(tokens, chosen, gates, capacity, w_gate, w_up, w_down):
    experts_n = lax.axis_size(EXPERT)
    ffn_n = lax.axis_size("ffn")
    me = lax.axis_index("ffn")
    tok_dev, width = tokens.shape
    picked_ids = chosen[0]
    listed = picked_ids.shape[0]
    slot_depth = 2 * listed // experts_n
    depth = slot_depth // ffn_n
    held = experts_n * depth

    positions = jnp.arange(listed, dtype=jnp.int32)
    alive = positions < capacity[0]
    weights = jnp.where(alive, gates[0], jnp.zeros_like(gates[0]))
    source = picked_ids // tok_dev
    offset = picked_ids - source * tok_dev
    member = one_hot(source, jnp.arange(experts_n, dtype=jnp.int32))
    earlier = (positions[:, None] > positions[None, :]).astype(jnp.bfloat16)
    before = mm(earlier, member)
    rank_in = jnp.sum(before * member.astype(jnp.float32), axis=1).astype(jnp.int32)
    place_in = (rank_in % ffn_n) * depth + rank_in // ffn_n
    asked = jnp.where(alive, offset + 1, 0).astype(jnp.bfloat16)
    spread = one_hot(place_in, jnp.arange(slot_depth, dtype=jnp.int32)) * asked[:, None]
    request = lax.dot_general(
        member, spread, (((0,), (0,)), ((), ())), preferred_element_type=jnp.float32
    )
    request = request.astype(jnp.int32) - 1
    requested = swap(request.reshape(experts_n, 1, slot_depth))
    requested = requested.reshape(experts_n, ffn_n, depth)

    pieces = jnp.stack([tokens, hop(tokens, 1), hop(tokens, 2), hop(tokens, -1)])

    mine = lax.dynamic_index_in_dim(requested, me, 1, keepdims=False).reshape(-1)
    selects = one_hot(mine, jnp.arange(tok_dev, dtype=jnp.int32))
    rows = jnp.concatenate(
        [
            mm(
                selects,
                lax.dynamic_index_in_dim(pieces, lax.rem(me + ffn_n - b, ffn_n), 0, keepdims=False),
            ).astype(jnp.bfloat16)
            for b in range(ffn_n)
        ],
        axis=1,
    )
    rows, own_down = lax.optimization_barrier((rows, w_down[0]))
    arrived = swap(rows.reshape(experts_n, depth, -1)).reshape(held, -1)

    own_gate, own_up = w_gate[0], w_up[0]
    shared = [own_gate, own_up, own_down]
    right_gate, right_up = hop(own_gate, -1), hop(own_up, -1)
    left = [hop(own_gate, 1), hop(own_up, 1), hop(own_down, 1)]
    right = [right_gate, right_up, hop(own_down, -1)]
    far = [hop(left[0], 1), hop(right[1], -1), hop(right[2], -1)]

    slot_of = source * depth + rank_in // ffn_n
    at_mine = (rank_in % ffn_n) == me
    gate_of = jnp.sum(
        jnp.where(
            (jnp.arange(held, dtype=jnp.int32)[:, None] == slot_of[None, :])
            & at_mine[None, :],
            weights[None, :],
            0.0,
        ),
        axis=1,
    )

    joined = []
    for k, dim in ((0, 1), (1, 1), (2, 0)):
        parts = [g[k] for g in (shared, left, right, far)]
        joined.append(jnp.concatenate(parts, axis=dim))
    gate_cols, up_cols, down_rows = lax.optimization_barrier(tuple(joined))
    hidden = (jax.nn.silu(mm(arrived, gate_cols)) * mm(arrived, up_cols)).astype(jnp.bfloat16)
    summed = mm(hidden, down_rows)
    contribution = (gate_of[:, None] * summed).astype(jnp.bfloat16)
    returned = swap(contribution.reshape(experts_n, depth, -1))

    tiles = jnp.moveaxis(returned.reshape(held, ffn_n, width), 1, 0)
    tiles = lax.all_to_all(tiles, "ffn", split_axis=0, concat_axis=0, tiled=True)
    slot_token = jnp.moveaxis(requested, 1, 0).reshape(-1)
    placement = one_hot(jnp.arange(tok_dev, dtype=jnp.int32), slot_token)
    return mm(placement, tiles.reshape(ffn_n * held, width)).astype(jnp.bfloat16)


def solution(mesh):
    split = Mesh(
        mesh.devices.reshape(
            mesh.shape["cfg"], mesh.shape["expert"] // 2, 2, mesh.shape["ffn"]
        ),
        ("cfg", "expert_0", "expert_1", "ffn"),
    )
    return jax.shard_map(
        shards,
        mesh=split,
        in_specs=(
            P(CFG_EXPERT, "ffn"),
            P(CFG_EXPERT, None),
            P(CFG_EXPERT, None),
            P("cfg"),
            P(EXPERT, None, "ffn"),
            P(EXPERT, None, "ffn"),
            P(EXPERT, "ffn", None),
        ),
        out_specs=P(CFG_EXPERT, "ffn"),
        check_vma=False,
    )
```
